64 devices in a mesh: dp: 8 (over x, y, core), sp: 8 (over z).
Axes of the slice: x: 2, y: 2, z: 8, core: 2. Of those that a mesh axis runs over, the one named last changes fastest.
The devices are a block of a 4x4x8 slice.
Arguments:
- x: bfloat16 [65536, 1152], P(('dp', 'sp')), parts along dimension 0
- gain: bfloat16 [1152], replicated
- wq: bfloat16 [1152, 1024], P('sp')
- wk: bfloat16 [1152, 256], P('sp')
- wv: bfloat16 [1152, 256], P('sp')
- wo: bfloat16 [1024, 1152], P('sp')
Outputs:
- output: bfloat16 [65536, 1152], P(('dp', 'sp')), parts along dimension 0
There are 8 independent parts. The reference program is written for one: setup_inputs(seed, part) draws one part's arguments, and reference() takes and returns one part's arrays. A program takes and returns all parts, laid end to end along the dimension named above; an argument that names none is the same for every part.
All inputs are finite; a program needn't handle non-finite values.
Results may differ from the reference program's by a relative error of at most 0.012.
Values are sent between devices in bfloat16 or wider.
A program may use at most 768 MiB of HBM per device.

```python
import jax
import jax.numpy as jnp
from jax import lax

ROWS = 8192
D = 1152
HEADS = 4
KV_HEADS = 1
HEAD = 256
THETA = 10000


def setup_inputs(seed: int = 0, part: int = 0) -> dict:
    kx, kn, kq, kk, kv, ko = jax.random.split(jax.random.key(seed), 6)

    def weights(key, rows, columns):
        return jax.random.normal(key, (rows, columns), jnp.float32) * rows**-0.5

    drawn = {
        "x": jax.random.normal(jax.random.fold_in(kx, part), (ROWS, D), jnp.float32),
        "gain": 1 + 0.1 * jax.random.normal(kn, (D,), jnp.float32),
        "wq": 2 * weights(kq, D, HEADS * HEAD),
        "wk": 2 * weights(kk, D, KV_HEADS * HEAD),
        "wv": 4 * weights(kv, D, KV_HEADS * HEAD),
        "wo": weights(ko, HEADS * HEAD, D),
    }
    return {k: v.astype(jnp.bfloat16) for k, v in drawn.items()}


def normed(x, gain):
    wide = x.astype(jnp.float32)
    scale = lax.rsqrt(jnp.mean(wide * wide, -1, keepdims=True) + 1e-6)
    return (wide * scale * gain.astype(jnp.float32)).astype(jnp.bfloat16)


def turned(t, place, theta):
    half = t.shape[-1] // 2
    angle = place.astype(jnp.float32)[:, None] * theta ** (-jnp.arange(half, dtype=jnp.float32) / half)
    cos, sin = jnp.cos(angle)[:, None], jnp.sin(angle)[:, None]
    a, b = t[..., :half].astype(jnp.float32), t[..., half:].astype(jnp.float32)
    return jnp.concatenate([a * cos - b * sin, b * cos + a * sin], -1).astype(jnp.bfloat16)


def matmul(a, w):
    return jnp.dot(a, w, preferred_element_type=jnp.float32).astype(jnp.bfloat16)


def einsum(form, a, b):
    return jnp.einsum(form, a.astype(jnp.float32), b.astype(jnp.float32))


def attention(q, k, v):
    scores = einsum("tgsd,ugd->gstu", q, k) * q.shape[-1] ** -0.5
    token = jnp.arange(q.shape[0])
    scores = jnp.where(token[:, None] >= token, scores, -jnp.inf)
    weights = jax.nn.softmax(scores, -1).astype(jnp.bfloat16)
    return einsum("gstu,ugd->tgsd", weights, v).astype(jnp.bfloat16)


def reference(x, gain, wq, wk, wv, wo):
    a, place = normed(x, gain), jnp.arange(ROWS)
    q = turned(matmul(a, wq).reshape(ROWS, HEADS, HEAD), place, THETA).reshape(ROWS, KV_HEADS, -1, HEAD)
    k = turned(matmul(a, wk).reshape(ROWS, KV_HEADS, HEAD), place, THETA)
    v = matmul(a, wv).reshape(ROWS, KV_HEADS, HEAD)
    seen = attention(q, k, v).reshape(ROWS, HEADS * HEAD)
    return (x.astype(jnp.float32) + jnp.dot(seen, wo, preferred_element_type=jnp.float32)).astype(jnp.bfloat16)
```

```python
import functools

import jax
import jax.numpy as jnp
from jax import lax
from jax.experimental import pallas as pl
from jax.experimental.pallas import tpu as pltpu
from jax.sharding import PartitionSpec as P

HEAD = 256
THETA = 10000
MESH = pl.DeviceIdType.MESH
HIDDEN = -2e30
LOG2E = 1.4426950408889634
CHUNK = 512
WIDE = 512
VMEM = 60 * 2**20


def _dot(a, b, ca, cb):
    return lax.dot_general(a, b, (((ca,), (cb,)), ((), ())), preferred_element_type=jnp.float32)


def _kernel(n, x_ref, gain_ref, freq_ref, wq_ref, wk_ref, wv_ref, wo_ref, y_ref,
            a_s, wkv_s, wq_s, wo_s, cos_s, sin_s, q_s, kv_s, top_s, mix_s, seen_s,
            w_send, w_recv, p_send, p_recv, kv_send, kv_recv):
    z = lax.axis_index("sp")
    dp = lax.axis_index("dp")
    core = lax.rem(dp, 2)
    partner = dp + 1 - 2 * core
    sign = 1 - 2 * core
    own = x_ref.shape[0]
    heads = wq_ref.shape[1] // HEAD
    half = HEAD // 2
    cols = heads * own
    hops = (n // 2, n - 1 - n // 2)
    chunks = own // CHUNK

    def at(steps):
        return lax.rem(z + sign * steps + 2 * n, n)

    def step_of(d):
        return 1 - 2 * d

    barrier = pltpu.get_barrier_semaphore()
    for target in ({"sp": at(1)}, {"sp": at(-1)}, {"dp": partner}):
        pl.semaphore_signal(barrier, inc=1, device_id=target, device_id_type=MESH)
    pl.semaphore_wait(barrier, 3)

    rk, ro = wk_ref.shape[0], wo_ref.shape[0]
    hq = wq_ref.shape[1] // 2
    ho = ro // 2

    def place(item, block, which):
        if item == 0:
            return wkv_s.at[which, pl.ds(pl.multiple_of(block * rk, 16), rk), :]
        if item == 1:
            return wq_s.at[which, pl.ds(pl.multiple_of(block * rk, 16), rk), :]
        return wo_s.at[pl.ds(pl.multiple_of(block * ro + which * ho, 16), ho), :]

    def w_copy(item, d, s, src=None):
        block = at(-s * step_of(d))
        dst = place(item, block, core)
        return pltpu.make_async_remote_copy(
            src_ref=dst if src is None else src, dst_ref=dst, send_sem=w_send.at[item, d, s], recv_sem=w_recv.at[item, d, s],
            device_id={"sp": at(step_of(d))}, device_id_type=MESH)

    def w_arrival(item, d, s):
        dst = place(item, at(-s * step_of(d)), core)
        return pltpu.make_async_remote_copy(
            src_ref=dst, dst_ref=dst, send_sem=w_send.at[item, d, s - 1], recv_sem=w_recv.at[item, d, s - 1],
            device_id={"sp": at(step_of(d))}, device_id_type=MESH)

    def p_copy(item, d, s):
        dst = place(item, at(-s * step_of(d)), core)
        return pltpu.make_async_remote_copy(
            src_ref=dst, dst_ref=dst, send_sem=p_send.at[item, d, s - 1], recv_sem=p_recv.at[item, d, s - 1],
            device_id={"dp": partner}, device_id_type=MESH)

    def p_arrival(item, d, s):
        dst = place(item, at(s * step_of(d)), 1 - core)
        return pltpu.make_async_remote_copy(
            src_ref=dst, dst_ref=dst, send_sem=p_send.at[item, d, s - 1], recv_sem=p_recv.at[item, d, s - 1],
            device_id={"dp": partner}, device_id_type=MESH)

    def own_wkv(start):
        for which, ref in ((0, wk_ref), (1, wv_ref)):
            @pl.when(core == which)
            def _():
                for d in (0, 1):
                    start(w_copy(0, d, 0, ref))

    def own_src(item):
        if item == 1:
            return wq_ref.at[:, pl.ds(pl.multiple_of(core * hq, 128), hq)]
        return wo_ref.at[pl.ds(pl.multiple_of(core * ho, 16), ho), :]

    def own_w(item):
        for d in (0, 1):
            w_copy(item, d, 0, own_src(item)).start()

    def w_hop(item, s):
        for d in (0, 1):
            if s <= hops[d]:
                w_arrival(item, d, s).wait_recv()
                if s < hops[d]:
                    w_copy(item, d, s).start()
                p_copy(item, d, s).start()

    def w_partner(item):
        for d in (0, 1):
            for s in range(1, hops[d] + 1):
                p_arrival(item, d, s).wait_recv()

    def kv_copy(d, s, c):
        ref = kv_s.at[at(-s * step_of(d)), c]
        return pltpu.make_async_remote_copy(
            src_ref=ref, dst_ref=ref, send_sem=kv_send.at[d, s, c], recv_sem=kv_recv.at[d, s, c],
            device_id={"sp": at(step_of(d))}, device_id_type=MESH)

    def kv_arrival(d, s, c):
        ref = kv_s.at[at(-s * step_of(d)), c]
        return pltpu.make_async_remote_copy(
            src_ref=ref, dst_ref=ref, send_sem=kv_send.at[d, s - 1, c], recv_sem=kv_recv.at[d, s - 1, c],
            device_id={"sp": at(step_of(d))}, device_id_type=MESH)

    rows = 128

    def normed(i, _):
        here = pl.ds(pl.multiple_of(i * rows, rows), rows)
        wide = x_ref[here, :].astype(jnp.float32)
        scale = lax.rsqrt(jnp.mean(wide * wide, -1, keepdims=True) + 1e-6)
        a_s[here, :] = (wide * scale * gain_ref[...].astype(jnp.float32)).astype(jnp.bfloat16)

    def tables(i, _):
        here = pl.ds(pl.multiple_of(i * rows, rows), rows)
        token = lax.broadcasted_iota(jnp.int32, (rows, half), 0) + (z * own + i * rows)
        angle = token.astype(jnp.float32) * freq_ref[...]
        cos_s[here, :] = jnp.cos(angle)
        sin_s[here, :] = jnp.sin(angle)

    def turned(t, here):
        t = t.astype(jnp.bfloat16).astype(jnp.float32)
        a, b = t[:, :half], t[:, half:]
        cos, sin = cos_s[here, :], sin_s[here, :]
        return jnp.concatenate([a * cos - b * sin, b * cos + a * sin], axis=1).astype(jnp.bfloat16)

    def keys_values(c):
        here = pl.ds(c * CHUNK, CHUNK)
        a = a_s[here, :]
        kv_s[z, c, :CHUNK, :] = turned(_dot(a, wkv_s[0], 1, 0), here)
        v = _dot(a, wkv_s[1], 1, 0).astype(jnp.bfloat16).T
        for i in range(CHUNK // HEAD):
            kv_s[z, c, CHUNK + i * HEAD : CHUNK + (i + 1) * HEAD, :] = v[:, i * HEAD : (i + 1) * HEAD]

    e = HEAD**-0.5 * LOG2E
    ones = jnp.ones((8, CHUNK), jnp.bfloat16)
    pieces = range(0, cols, WIDE)

    def block(b, c, which, masked, first):
        k = kv_s[b, c, :CHUNK, :]
        v = jnp.concatenate([kv_s[b, c, CHUNK + i * HEAD : CHUNK + (i + 1) * HEAD, :] for i in range(CHUNK // HEAD)], axis=1)
        values = jnp.concatenate([v, ones], axis=0)
        scores = [_dot(k, q_s[p : p + WIDE, :], 1, 1) for p in which]
        weights, keeps = [], []
        for p, s in zip(which, scores):
            if p in masked:
                key = lax.broadcasted_iota(jnp.int32, s.shape, 0) + c * CHUNK
                query = lax.broadcasted_iota(jnp.int32, s.shape, 1) + p % own
                s = jnp.where(query >= key, s, HIDDEN)
            top = s.max(axis=0, keepdims=True)
            if first:
                keeps.append(None)
            else:
                old = top_s[:, p : p + WIDE]
                top = jnp.maximum(old, top)
                keeps.append(jnp.exp2((old - top) * e))
            top_s[:, p : p + WIDE] = top
            weights.append(jnp.exp2((s - top) * e).astype(jnp.bfloat16))
        for p, w, keep in zip(which, weights, keeps):
            got = _dot(values, w, 1, 0)
            mix_s[:, p : p + WIDE] = got if first else mix_s[:, p : p + WIDE] * keep + got

    own_wkv(lambda copy: copy.start())
    own_w(1)
    wkv_s[0, pl.ds(pl.multiple_of(z * rk, 16), rk), :] = wk_ref[...]
    wkv_s[1, pl.ds(pl.multiple_of(z * rk, 16), rk), :] = wv_ref[...]
    for i in range(2):
        wq_s[i, pl.ds(pl.multiple_of(z * rk, 16), rk), :] = wq_ref[:, i * hq : (i + 1) * hq]
    wo_s[pl.ds(pl.multiple_of(z * ro, 16), ro), :] = wo_ref[...]
    steps = own // rows
    lax.fori_loop(0, steps // 2, normed, None)
    w_hop(0, 1)
    own_w(2)
    lax.fori_loop(steps // 2, steps, normed, None)
    w_hop(0, 2)
    w_hop(1, 1)
    lax.fori_loop(0, steps // 2, tables, None)
    w_hop(0, 3)
    w_hop(2, 1)
    lax.fori_loop(steps // 2, steps, tables, None)
    w_hop(0, 4)
    w_partner(0)
    w_hop(1, 2)
    for c in range(chunks):
        keys_values(c)
        w_hop(2, 2) if c == 0 else w_hop(1, 3)
        for d in (0, 1):
            kv_copy(d, 0, c).start()
    w_hop(2, 3)
    w_hop(1, 4)
    w_partner(1)
    for i in range(2):
        per = heads // 2
        for c in range(chunks):
            here = pl.ds(c * CHUNK, CHUNK)
            q = _dot(a_s[here, :], wq_s[i], 1, 0)
            for h in range(per):
                q_s[pl.ds((i * per + h) * own + c * CHUNK, CHUNK), :] = turned(q[:, h * HEAD : (h + 1) * HEAD], here)

    block(z, 0, [p for p in pieces], [p for p in pieces if p % own < CHUNK], True)
    for c in range(1, chunks):
        block(z, c, [p for p in pieces if p % own >= c * CHUNK], [p for p in pieces if c * CHUNK <= p % own < (c + 1) * CHUNK], False)

    both = 2 * chunks * hops[1]

    def arrive(i, _):
        late = i >= both
        s = jnp.where(late, hops[0], 1 + lax.div(i, 2 * chunks))
        c = jnp.where(late, i - both, lax.div(lax.rem(i, 2 * chunks), 2))
        d = jnp.where(late, 0, lax.rem(i, 2))
        kv_arrival(d, s, c).wait_recv()

        @pl.when(s < hops[0] - d)
        def _():
            kv_copy(d, s, c).start()

        b = at(-s * step_of(d))

        @pl.when(b < z)
        def _():
            block(b, c, [p for p in pieces], [], False)

    lax.fori_loop(0, both + chunks * (hops[0] - hops[1]), arrive, None)

    w_hop(2, 4)
    w_partner(2)
    for p in pieces:
        h, t = divmod(p, own)
        total = mix_s[HEAD : HEAD + 1, p : p + WIDE]
        seen_s[h * HEAD : (h + 1) * HEAD, t : t + WIDE] = (mix_s[:HEAD, p : p + WIDE] * (1 / total)).astype(jnp.bfloat16)
    tile = 256

    def project(i, _):
        here = pl.ds(pl.multiple_of(i * tile, tile), tile)
        got = _dot(seen_s[:, here], wo_s[...], 0, 0)
        y_ref[here, :] = (x_ref[here, :].astype(jnp.float32) + got).astype(jnp.bfloat16)

    lax.fori_loop(0, own // tile, project, None)

    own_wkv(lambda copy: copy.wait_send())
    for item in range(3):
        for d in (0, 1):
            if item:
                w_copy(item, d, 0, own_src(item)).wait_send()
            for s in range(1, hops[d] + 1):
                if s < hops[d]:
                    w_copy(item, d, s).wait_send()
                p_copy(item, d, s).wait_send()
    for d in (0, 1):
        for s in range(hops[d]):
            for c in range(chunks):
                kv_copy(d, s, c).wait_send()


def solution(mesh):
    n = mesh.shape["sp"]

    def step(x, gain, wq, wk, wv, wo):
        own, width = x.shape
        heads = wq.shape[1] // HEAD
        half = HEAD // 2
        freq = THETA ** (-jnp.arange(half, dtype=jnp.float32) / half)
        bf, f32 = jnp.bfloat16, jnp.float32
        vmem = pl.BlockSpec(memory_space=pltpu.VMEM)
        hops = n // 2
        return pl.pallas_call(
            functools.partial(_kernel, n),
            name="layer",
            out_shape=jax.ShapeDtypeStruct((own, width), bf),
            in_specs=[vmem] * 7,
            out_specs=vmem,
            scratch_shapes=[
                pltpu.VMEM((own, width), bf),
                pltpu.VMEM((2, width, HEAD), bf),
                pltpu.VMEM((2, width, wq.shape[1] // 2), bf),
                pltpu.VMEM((wq.shape[1], width), bf),
                pltpu.VMEM((own, half), f32),
                pltpu.VMEM((own, half), f32),
                pltpu.VMEM((heads * own, HEAD), bf),
                pltpu.VMEM((n, own // CHUNK, 2 * CHUNK, HEAD), bf),
                pltpu.VMEM((1, heads * own), f32),
                pltpu.VMEM((HEAD + 8, heads * own), f32),
                pltpu.VMEM((heads * HEAD, own), bf),
                pltpu.SemaphoreType.DMA((3, 2, hops)),
                pltpu.SemaphoreType.DMA((3, 2, hops)),
                pltpu.SemaphoreType.DMA((3, 2, hops)),
                pltpu.SemaphoreType.DMA((3, 2, hops)),
                pltpu.SemaphoreType.DMA((2, hops, own // CHUNK)),
                pltpu.SemaphoreType.DMA((2, hops, own // CHUNK)),
            ],
            compiler_params=pltpu.CompilerParams(collective_id=0, has_side_effects=True, vmem_limit_bytes=VMEM),
        )(x, gain[None], freq[None], wq, wk, wv, wo)

    tokens, whole = P(("dp", "sp"), None), P("sp", None)
    return jax.shard_map(
        step,
        mesh=mesh,
        in_specs=(tokens, P(None), whole, whole, whole, whole),
        out_specs=tokens,
        check_vma=False,
    )
```

```python
import functools

import jax
import jax.numpy as jnp
import numpy as np
from jax import lax
from jax.experimental import pallas as pl
from jax.experimental.pallas import tpu as pltpu
from jax.sharding import PartitionSpec as P

HEAD = 256
THETA = 10000
MESH = pl.DeviceIdType.MESH
HIDDEN = -2e30
LOG2E = 1.4426950408889634
CHUNK = 512
WIDE = 512
TILE = 256
VMEM = 40 * 2**20


def _dot(a, b, ca, cb):
    return lax.dot_general(a, b, (((ca,), (cb,)), ((), ())), preferred_element_type=jnp.float32)


def _kernel(n, x_hbm, gain_ref, freq_ref, wq_ref, wk_ref, wv_ref, wo_ref, seen_s, wo_s,
            x_ref, a_s, wkv_s, wq_s, cos_s, sin_s, q_s, kv_s, top_s, mix_s,
            x_sem, w_send, w_recv, p_send, p_recv, y_send, y_recv, r_send, r_recv, kv_send, kv_recv):
    z = lax.axis_index("sp")
    dp = lax.axis_index("dp")
    core = lax.rem(dp, 2)
    side = lax.rem(lax.div(dp, 2), 2)
    partner = dp + 1 - 2 * core
    across = dp + 2 - 4 * side
    sign = 1 - 2 * core
    load = pltpu.make_async_copy(x_hbm, x_ref, x_sem)
    load.start()
    own = x_ref.shape[0]
    heads = wq_ref.shape[1] // HEAD
    half = HEAD // 2
    cols = heads * own
    hops = (n // 2, n - 1 - n // 2)
    chunks = own // CHUNK

    def at(steps):
        return lax.rem(z + sign * steps + 2 * n, n)

    def step_of(d):
        return 1 - 2 * d

    barrier = pltpu.get_barrier_semaphore()
    for target in ({"sp": at(1)}, {"sp": at(-1)}, {"dp": partner}, {"dp": across}):
        pl.semaphore_signal(barrier, inc=1, device_id=target, device_id_type=MESH)
    pl.semaphore_wait(barrier, 4)

    rk, ro = wk_ref.shape[0], wo_ref.shape[0]
    hq = wq_ref.shape[1] // 4
    ho = ro // 4

    def part(item, c, s):
        return c if item == 0 else c + 2 * s

    def place(item, block, which):
        if item == 0:
            return wkv_s.at[which, pl.ds(pl.multiple_of(block * rk, 16), rk), :]
        if item == 1:
            return wq_s.at[which, pl.ds(pl.multiple_of(block * rk, 16), rk), :]
        return wo_s.at[pl.ds(pl.multiple_of(block * ro + which * ho, 16), ho), :]

    def w_copy(item, d, s, src=None):
        block = at(-s * step_of(d))
        dst = place(item, block, part(item, core, side))
        return pltpu.make_async_remote_copy(
            src_ref=dst if src is None else src, dst_ref=dst, send_sem=w_send.at[item, d, s], recv_sem=w_recv.at[item, d, s],
            device_id={"sp": at(step_of(d))}, device_id_type=MESH)

    def w_arrival(item, d, s):
        dst = place(item, at(-s * step_of(d)), part(item, core, side))
        return pltpu.make_async_remote_copy(
            src_ref=dst, dst_ref=dst, send_sem=w_send.at[item, d, s - 1], recv_sem=w_recv.at[item, d, s - 1],
            device_id={"sp": at(step_of(d))}, device_id_type=MESH)

    def p_copy(item, d, s):
        dst = place(item, at(-s * step_of(d)), part(item, core, side))
        return pltpu.make_async_remote_copy(
            src_ref=dst, dst_ref=dst, send_sem=p_send.at[item, d, s - 1], recv_sem=p_recv.at[item, d, s - 1],
            device_id={"dp": partner}, device_id_type=MESH)

    def p_arrival(item, d, s):
        dst = place(item, at(s * step_of(d)), part(item, 1 - core, side))
        return pltpu.make_async_remote_copy(
            src_ref=dst, dst_ref=dst, send_sem=p_send.at[item, d, s - 1], recv_sem=p_recv.at[item, d, s - 1],
            device_id={"dp": partner}, device_id_type=MESH)

    def y_copy(item, d, s):
        dst = place(item, at(-s * step_of(d)), part(item, core, side))
        return pltpu.make_async_remote_copy(
            src_ref=dst, dst_ref=dst, send_sem=y_send.at[item, d, s - 1], recv_sem=y_recv.at[item, d, s - 1],
            device_id={"dp": across}, device_id_type=MESH)

    def y_arrival(item, d, s):
        dst = place(item, at(-s * step_of(d)), part(item, core, 1 - side))
        return pltpu.make_async_remote_copy(
            src_ref=dst, dst_ref=dst, send_sem=y_send.at[item, d, s - 1], recv_sem=y_recv.at[item, d, s - 1],
            device_id={"dp": across}, device_id_type=MESH)

    def r_copy(item, d, s):
        dst = place(item, at(-s * step_of(d)), part(item, core, 1 - side))
        return pltpu.make_async_remote_copy(
            src_ref=dst, dst_ref=dst, send_sem=r_send.at[item, d, s - 1], recv_sem=r_recv.at[item, d, s - 1],
            device_id={"dp": partner}, device_id_type=MESH)

    def r_arrival(item, d, s):
        dst = place(item, at(s * step_of(d)), part(item, 1 - core, 1 - side))
        return pltpu.make_async_remote_copy(
            src_ref=dst, dst_ref=dst, send_sem=r_send.at[item, d, s - 1], recv_sem=r_recv.at[item, d, s - 1],
            device_id={"dp": partner}, device_id_type=MESH)

    def own_wkv(start):
        for which, ref in ((0, wk_ref), (1, wv_ref)):
            @pl.when(core == which)
            def _():
                for d in (0, 1):
                    start(w_copy(0, d, 0, ref))

    def own_src(item):
        if item == 1:
            return wq_ref.at[:, pl.ds(pl.multiple_of(part(1, core, side) * hq, 128), hq)]
        return wo_ref.at[pl.ds(pl.multiple_of(part(2, core, side) * ho, 16), ho), :]

    def own_w(item):
        for d in (0, 1):
            w_copy(item, d, 0, own_src(item)).start()

    def w_hop(item, s):
        for d in (0, 1):
            if s <= hops[d]:
                w_arrival(item, d, s).wait_recv()
                if s < hops[d]:
                    w_copy(item, d, s).start()
                p_copy(item, d, s).start()
                if item:
                    y_copy(item, d, s).start()

    def w_relay(item, s):
        for d in (0, 1):
            if s <= hops[d]:
                y_arrival(item, d, s).wait_recv()
                r_copy(item, d, s).start()

    def w_partner(item):
        for d in (0, 1):
            for s in range(1, hops[d] + 1):
                p_arrival(item, d, s).wait_recv()
                if item:
                    r_arrival(item, d, s).wait_recv()

    def kv_copy(d, s, c):
        ref = kv_s.at[at(-s * step_of(d)), c]
        return pltpu.make_async_remote_copy(
            src_ref=ref, dst_ref=ref, send_sem=kv_send.at[d, s, c], recv_sem=kv_recv.at[d, s, c],
            device_id={"sp": at(step_of(d))}, device_id_type=MESH)

    def kv_arrival(d, s, c):
        ref = kv_s.at[at(-s * step_of(d)), c]
        return pltpu.make_async_remote_copy(
            src_ref=ref, dst_ref=ref, send_sem=kv_send.at[d, s - 1, c], recv_sem=kv_recv.at[d, s - 1, c],
            device_id={"sp": at(step_of(d))}, device_id_type=MESH)

    rows = 128

    def normed(i, _):
        here = pl.ds(pl.multiple_of(i * rows, rows), rows)
        wide = x_ref[here, :].astype(jnp.float32)
        scale = lax.rsqrt(jnp.mean(wide * wide, -1, keepdims=True) + 1e-6)
        a_s[here, :] = (wide * scale * gain_ref[...].astype(jnp.float32).reshape(1, -1)).astype(jnp.bfloat16)

    def tables(i, _):
        here = pl.ds(pl.multiple_of(i * rows, rows), rows)
        token = lax.broadcasted_iota(jnp.int32, (rows, half), 0) + (z * own + i * rows)
        angle = token.astype(jnp.float32) * freq_ref[...]
        cos_s[here, :] = jnp.cos(angle)
        sin_s[here, :] = jnp.sin(angle)

    def turned(t, here):
        t = t.astype(jnp.bfloat16).astype(jnp.float32)
        a, b = t[:, :half], t[:, half:]
        cos, sin = cos_s[here, :], sin_s[here, :]
        return jnp.concatenate([a * cos - b * sin, b * cos + a * sin], axis=1).astype(jnp.bfloat16)

    def keys_values(c):
        here = pl.ds(c * CHUNK, CHUNK)
        a = a_s[here, :]
        kv_s[z, c, :CHUNK, :] = turned(_dot(a, wkv_s[0], 1, 0), here)
        v = _dot(a, wkv_s[1], 1, 0).astype(jnp.bfloat16).T
        for i in range(CHUNK // HEAD):
            kv_s[z, c, CHUNK + i * HEAD : CHUNK + (i + 1) * HEAD, :] = v[:, i * HEAD : (i + 1) * HEAD]

    e = HEAD**-0.5 * LOG2E
    ones = jnp.ones((8, CHUNK), jnp.bfloat16)
    pieces = range(0, cols, WIDE)

    def block(b, c, which, masked, first):
        k = kv_s[b, c, :CHUNK, :]
        v = jnp.concatenate([kv_s[b, c, CHUNK + i * HEAD : CHUNK + (i + 1) * HEAD, :] for i in range(CHUNK // HEAD)], axis=1)
        values = jnp.concatenate([v, ones], axis=0)
        scores = [_dot(k, q_s[p : p + WIDE, :], 1, 1) for p in which]
        weights, keeps = [], []
        for p, s in zip(which, scores):
            if p in masked:
                key = lax.broadcasted_iota(jnp.int32, s.shape, 0) + c * CHUNK
                query = lax.broadcasted_iota(jnp.int32, s.shape, 1) + p % own
                s = jnp.where(query >= key, s, HIDDEN)
            top = s.max(axis=0, keepdims=True)
            if first:
                keeps.append(None)
            else:
                old = top_s[:, p : p + WIDE]
                top = jnp.maximum(old, top)
                keeps.append(jnp.exp2((old - top) * e))
            top_s[:, p : p + WIDE] = top
            weights.append(jnp.exp2((s - top) * e).astype(jnp.bfloat16))
        for p, w, keep in zip(which, weights, keeps):
            got = _dot(values, w, 1, 0)
            mix_s[:, p : p + WIDE] = got if first else mix_s[:, p : p + WIDE] * keep + got

    own_wkv(lambda copy: copy.start())
    own_w(1)
    wkv_s[0, pl.ds(pl.multiple_of(z * rk, 16), rk), :] = wk_ref[...]
    wkv_s[1, pl.ds(pl.multiple_of(z * rk, 16), rk), :] = wv_ref[...]
    for i in range(4):
        wq_s[i, pl.ds(pl.multiple_of(z * rk, 16), rk), :] = wq_ref[:, i * hq : (i + 1) * hq]
    wo_s[pl.ds(pl.multiple_of(z * ro, 16), ro), :] = wo_ref[...]
    steps = own // rows
    load.wait()
    lax.fori_loop(0, steps // 2, normed, None)
    w_hop(0, 1)
    w_hop(1, 1)
    lax.fori_loop(steps // 2, steps, normed, None)
    w_hop(0, 2)
    w_hop(1, 2)
    w_relay(1, 1)
    lax.fori_loop(0, steps // 2, tables, None)
    w_hop(0, 3)
    w_hop(1, 3)
    own_w(2)
    w_relay(1, 2)
    lax.fori_loop(steps // 2, steps, tables, None)
    w_hop(0, 4)
    w_partner(0)
    for c in range(chunks):
        keys_values(c)
        w_hop(1, 4) if c == 0 else w_hop(2, 1)
        for d in (0, 1):
            kv_copy(d, 0, c).start()
    w_relay(1, 3)
    w_relay(1, 4)
    w_partner(1)
    for i in range(4):
        per = heads // 4
        for c in range(chunks):
            here = pl.ds(c * CHUNK, CHUNK)
            q = _dot(a_s[here, :], wq_s[i], 1, 0)
            for h in range(per):
                q_s[pl.ds((i * per + h) * own + c * CHUNK, CHUNK), :] = turned(q[:, h * HEAD : (h + 1) * HEAD], here)

    block(z, 0, [p for p in pieces], [p for p in pieces if p % own < CHUNK], True)
    for c in range(1, chunks):
        block(z, c, [p for p in pieces if p % own >= c * CHUNK], [p for p in pieces if c * CHUNK <= p % own < (c + 1) * CHUNK], False)

    both = 2 * chunks * hops[1]

    def arrive(i, _):
        late = i >= both
        s = jnp.where(late, hops[0], 1 + lax.div(i, 2 * chunks))
        c = jnp.where(late, i - both, lax.div(lax.rem(i, 2 * chunks), 2))
        d = jnp.where(late, 0, lax.rem(i, 2))
        kv_arrival(d, s, c).wait_recv()

        @pl.when(s < hops[0] - d)
        def _():
            kv_copy(d, s, c).start()

        for hop in range(2, hops[0] + 1):
            @pl.when(i == 2 * chunks * (hop - 2) + 1)
            def _():
                w_hop(2, hop)
                w_relay(2, hop - 1)

        b = at(-s * step_of(d))

        @pl.when(b < z)
        def _():
            block(b, c, [p for p in pieces], [], False)

    lax.fori_loop(0, both + chunks * (hops[0] - hops[1]), arrive, None)

    w_relay(2, hops[0])
    for p in pieces:
        h, t = divmod(p, own)
        total = mix_s[HEAD : HEAD + 1, p : p + WIDE]
        seen_s[h * HEAD : (h + 1) * HEAD, t : t + WIDE] = (mix_s[:HEAD, p : p + WIDE] * (1 / total)).astype(jnp.bfloat16)
    w_partner(2)

    own_wkv(lambda copy: copy.wait_send())
    for item in range(3):
        for d in (0, 1):
            if item:
                w_copy(item, d, 0, own_src(item)).wait_send()
            for s in range(1, hops[d] + 1):
                if s < hops[d]:
                    w_copy(item, d, s).wait_send()
                p_copy(item, d, s).wait_send()
                if item:
                    y_copy(item, d, s).wait_send()
                    r_copy(item, d, s).wait_send()
    for d in (0, 1):
        for s in range(hops[d]):
            for c in range(chunks):
                kv_copy(d, s, c).wait_send()


def _project(x_ref, seen_ref, wo_ref, y_ref):
    here = pl.ds(pl.multiple_of(pl.program_id(0) * TILE, TILE), TILE)
    got = _dot(seen_ref[:, here], wo_ref[...], 0, 0)
    y_ref[...] = (x_ref[...].astype(jnp.float32) + got).astype(jnp.bfloat16)


def solution(mesh):
    n = mesh.shape["sp"]

    def step(x, gain, wq, wk, wv, wo):
        own, width = x.shape
        heads = wq.shape[1] // HEAD
        half = HEAD // 2
        freq = np.float32(THETA) ** (-np.arange(half, dtype=np.float32) / np.float32(half))
        bf, f32 = jnp.bfloat16, jnp.float32
        vmem = pl.BlockSpec(memory_space=pltpu.VMEM)
        hops = n // 2
        dma = pltpu.SemaphoreType.DMA((3, 2, hops))
        seen, wo = pl.pallas_call(
            functools.partial(_kernel, n),
            name="attend",
            out_shape=[pltpu.VMEM((wq.shape[1], own), bf), pltpu.VMEM((wq.shape[1], width), bf)],
            in_specs=[pl.BlockSpec(memory_space=pltpu.HBM)] + [vmem] * 6,
            out_specs=[vmem, vmem],
            scratch_shapes=[
                pltpu.VMEM((own, width), bf),
                pltpu.VMEM((own, width), bf),
                pltpu.VMEM((2, width, HEAD), bf),
                pltpu.VMEM((4, width, wq.shape[1] // 4), bf),
                pltpu.VMEM((own, half), f32),
                pltpu.VMEM((own, half), f32),
                pltpu.VMEM((heads * own, HEAD), bf),
                pltpu.VMEM((n, own // CHUNK, 2 * CHUNK, HEAD), bf),
                pltpu.VMEM((1, heads * own), f32),
                pltpu.VMEM((HEAD + 8, heads * own), f32),
                pltpu.SemaphoreType.DMA,
                *[dma] * 8,
                pltpu.SemaphoreType.DMA((2, hops, own // CHUNK)),
                pltpu.SemaphoreType.DMA((2, hops, own // CHUNK)),
            ],
            compiler_params=pltpu.CompilerParams(collective_id=0, has_side_effects=True, vmem_limit_bytes=VMEM),
        )(*(pltpu.with_memory_space_constraint(t, pltpu.HBM) for t in (x, gain, jnp.asarray(freq[None]), wq, wk, wv, wo)))
        tile = pl.BlockSpec((TILE, width), lambda i: (i, 0))
        return pl.pallas_call(
            _project,
            name="project",
            out_shape=jax.ShapeDtypeStruct((own, width), bf),
            grid=(own // TILE,),
            in_specs=[tile, vmem, vmem],
            out_specs=tile,
            compiler_params=pltpu.CompilerParams(dimension_semantics=("arbitrary",), vmem_limit_bytes=16 * 2**20),
        )(x, seen, wo)

    tokens, whole = P(("dp", "sp"), None), P("sp", None)
    return jax.shard_map(
        step,
        mesh=mesh,
        in_specs=(tokens, P(None), whole, whole, whole, whole),
        out_specs=tokens,
        check_vma=False,
    )
```

```python
import functools
import math

import jax
import jax.numpy as jnp
import numpy as np
from jax import lax
from jax.experimental import pallas as pl
from jax.experimental.pallas import tpu as pltpu
from jax.sharding import PartitionSpec as P

HEAD = 256
THETA = 10000
MESH = pl.DeviceIdType.MESH
HIDDEN = -2e30
LOG2E = 1.4426950408889634
CHUNK = 512
PART = 256
WIDE = 512
TILE = 256
VMEM = 40 * 2**20


def _dot(a, b, ca, cb):
    return lax.dot_general(a, b, (((ca,), (cb,)), ((), ())), preferred_element_type=jnp.float32)


def _kernel(n, row, x_hbm, gain_hbm, freq_hbm, wq_hbm, wk_hbm, wv_hbm, wo_hbm, seen_s, wo_s,
            x_ref, gain_ref, freq_ref, a_s, wkv_s, wq_s, cos_s, sin_s, q_s, kv_s, top_s, mix_s,
            load_sem, z_send, z_recv, x_send, x_recv, y_send, y_recv, p_send, p_recv, kv_send, kv_recv):
    z = lax.axis_index("sp")
    dp = lax.axis_index("dp")
    core = lax.rem(dp, 2)
    ys = lax.rem(lax.div(dp, 2), 2)
    xs = lax.rem(lax.div(dp, row), 2)
    partner = dp + 1 - 2 * core
    across = dp + 2 - 4 * ys
    beside = dp + row - 2 * row * xs
    sign = 1 - 2 * core
    own = x_ref.shape[0]
    heads = wq_hbm.shape[1] // HEAD
    half = HEAD // 2
    cols = heads * own
    hops = (n // 2, n - 1 - n // 2)
    chunks = own // CHUNK

    def at(steps):
        return lax.rem(z + sign * steps + 2 * n, n)

    def step_of(d):
        return 1 - 2 * d

    rk, ro = wk_hbm.shape[0], wo_hbm.shape[0]
    own_rows = pl.ds(pl.multiple_of(z * rk, 16), rk)
    loads = [
        pltpu.make_async_copy(src, dst, load_sem.at[i])
        for i, (src, dst) in enumerate((
            (wk_hbm, wkv_s.at[0, own_rows, :]), (wv_hbm, wkv_s.at[1, own_rows, :]), (wq_hbm, wq_s.at[own_rows, :]),
            (wo_hbm, wo_s.at[pl.ds(pl.multiple_of(z * ro, 16), ro), :]), (gain_hbm, gain_ref), (freq_hbm, freq_ref), (x_hbm, x_ref)))
    ]
    for load in loads:
        load.start()

    barrier = pltpu.get_barrier_semaphore()
    greeted = [{"sp": at(k)} for k in (2, -2, 1, -1)] + [{"dp": partner}, {"dp": across}, {"dp": beside}]
    for target in greeted:
        pl.semaphore_signal(barrier, inc=1, device_id=target, device_id_type=MESH)
    pl.semaphore_wait(barrier, len(greeted))

    hq, ho = wq_hbm.shape[1] // 8, ro // 8

    def lot(c, y, x, level):
        return (4 * c + 2 * y + x, 1) if level == 0 else (4 * c + 2 * y, 2) if level == 1 else (4 * c, 4)

    def place(item, block, c, y, x, level):
        first, count = lot(c, y, x, level)
        if item == 0:
            here = pl.ds(pl.multiple_of(block * rk, 16), rk)
            return wkv_s.at[c, here, :] if level == 2 else wkv_s.at[c, here, pl.ds(pl.multiple_of(y * half, 128), half)]
        if item == 1:
            return wq_s.at[pl.ds(pl.multiple_of(block * rk, 16), rk), pl.ds(pl.multiple_of(first * hq, 128), count * hq)]
        return wo_s.at[pl.ds(pl.multiple_of(block * ro + first * ho, 16), count * ho), :]

    def copy(dst, send, recv, target):
        return pltpu.make_async_remote_copy(
            src_ref=dst, dst_ref=dst, send_sem=send, recv_sem=recv, device_id=target, device_id_type=MESH)

    def block_of(d, s):
        return at(-s * step_of(d))

    def z_copy(item, d, s):
        came = (0 if s <= 2 else 2) if item == 0 else s - 1
        return copy(place(item, block_of(d, came), core, ys, xs, 0), z_send.at[item], z_recv.at[item, d, s - 1],
                    {"sp": at(step_of(d) * (s - came))})

    def z_arrival(item, d, s):
        return copy(place(item, block_of(d, s), core, ys, xs, 0), z_send.at[item], z_recv.at[item, d, s - 1], {"sp": at(step_of(d))})

    def x_copy(item, d, s):
        return copy(place(item, block_of(d, s), core, ys, xs, 0), x_send.at[item - 1], x_recv.at[item - 1, s - 1], {"dp": beside})

    def y_copy(item, d, s):
        return copy(place(item, block_of(d, s), core, ys, xs, 1), y_send.at[item], y_recv.at[item, s - 1], {"dp": across})

    def p_copy(item, d, s):
        return copy(place(item, block_of(d, s), core, ys, xs, 2), p_send.at[item], p_recv.at[item], {"dp": partner})

    def some_of(item, level, count):
        if item == 0:
            return wkv_s.at[0, : count * rk, :] if level == 2 else wkv_s.at[0, : count * rk, :half]
        if item == 1:
            return wq_s.at[: count * rk, : hq << level]
        return wo_s.at[: count * (ho << level), :]

    def wait_all(item, level, count, sem):
        ref = some_of(item, level, count)
        pltpu.make_async_copy(ref, ref, sem).wait()

    def each(s):
        return [d for d in (0, 1) if s <= hops[d]]

    def own_w(item):
        for s in (2, 1) if item == 0 else (1,):
            for d in (0, 1):
                z_copy(item, d, s).start()

    def z_hop(item, s):
        for d in each(s):
            z_arrival(item, d, s).wait_recv()
            for t in range(hops[d], 2, -1) if item == 0 and s == 2 else (s + 1,) if item and s < hops[d] else ():
                z_copy(item, d, t).start()
            (x_copy if item else y_copy)(item, d, s).start()

    def x_hop(item, s):
        wait_all(item, 0, len(each(s)), x_recv.at[item - 1, s - 1])
        for d in each(s):
            y_copy(item, d, s).start()

    def y_hop(item, s):
        wait_all(item, 1, len(each(s)), y_recv.at[item, s - 1])
        for d in each(s):
            p_copy(item, d, s).start()

    def p_hops(item):
        wait_all(item, 2, n - 1, p_recv.at[item])

    def kv_copy(d, s, c):
        return copy(kv_s.at[block_of(d, s), c], kv_send, kv_recv.at[d, s, c], {"sp": at(step_of(d))})

    def kv_arrival(d, s, c):
        return copy(kv_s.at[block_of(d, s), c], kv_send, kv_recv.at[d, s - 1, c], {"sp": at(step_of(d))})

    def kv_last(i, s):
        return copy(kv_s.at[block_of(0, s), chunks - 1, i], kv_send, kv_recv.at[1, hops[0] - 1, i], {"sp": at(1)})

    rows = 128

    def normed(i, _):
        here = pl.ds(pl.multiple_of(i * rows, rows), rows)
        wide = x_ref[here, :].astype(jnp.float32)
        scale = lax.rsqrt(jnp.mean(wide * wide, -1, keepdims=True) + 1e-6)
        a_s[here, :] = (wide * scale * gain_ref[...].astype(jnp.float32).reshape(1, -1)).astype(jnp.bfloat16)

    def tables(i, _):
        here = pl.ds(pl.multiple_of(i * rows, rows), rows)
        token = lax.broadcasted_iota(jnp.int32, (rows, half), 0) + (z * own + i * rows)
        angle = token.astype(jnp.float32) * freq_ref[...]
        cos_s[here, :] = jnp.cos(angle)
        sin_s[here, :] = jnp.sin(angle)

    def turned(t, here):
        t = t.astype(jnp.bfloat16).astype(jnp.float32)
        a, b = t[:, :half], t[:, half:]
        cos, sin = cos_s[here, :], sin_s[here, :]
        return jnp.concatenate([a * cos - b * sin, b * cos + a * sin], axis=1).astype(jnp.bfloat16)

    def keys_values(c):
        here = pl.ds(c * CHUNK, CHUNK)
        a = a_s[here, :]
        k = turned(_dot(a, wkv_s[0], 1, 0), here)
        v = _dot(a, wkv_s[1], 1, 0).astype(jnp.bfloat16).T
        for i in range(CHUNK // PART):
            kv_s[z, c, i, :PART, :] = k[i * PART : (i + 1) * PART, :]
            kv_s[z, c, i, PART:, :] = v[:, i * PART : (i + 1) * PART]

    e = HEAD**-0.5 * LOG2E
    pieces = range(0, cols, WIDE)

    def block(b, c, which, masked, first, parts=range(CHUNK // PART)):
        k = jnp.concatenate([kv_s[b, c, i, :PART, :] for i in parts], axis=0)
        v = jnp.concatenate([kv_s[b, c, i, PART:, :] for i in parts], axis=1)
        values = jnp.concatenate([v, jnp.ones((8, v.shape[1]), v.dtype)], axis=0)
        scores = [_dot(k, q_s[p : p + WIDE, :], 1, 1) for p in which]
        weights, keeps = [], []
        for p, s in zip(which, scores):
            if p in masked:
                key = lax.broadcasted_iota(jnp.int32, s.shape, 0) + c * CHUNK
                query = lax.broadcasted_iota(jnp.int32, s.shape, 1) + p % own
                s = jnp.where(query >= key, s, HIDDEN)
            top = s.max(axis=0, keepdims=True)
            if first:
                keeps.append(None)
            else:
                old = top_s[:, p : p + WIDE]
                top = jnp.maximum(old, top)
                keeps.append(jnp.exp2((old - top) * e))
            top_s[:, p : p + WIDE] = top
            weights.append(jnp.exp2((s - top) * e).astype(jnp.bfloat16))
        for p, w, keep in zip(which, weights, keeps):
            got = _dot(values, w, 1, 0)
            mix_s[:, p : p + WIDE] = got if first else mix_s[:, p : p + WIDE] * keep + got

    some = own // rows // 4

    def quarter(do, i):
        lax.fori_loop(i * some, (i + 1) * some, do, None)

    loads[0].wait()
    loads[1].wait()
    own_w(0)
    loads[2].wait()
    own_w(1)
    loads[3].wait()
    own_w(2)
    for load in loads[4:]:
        load.wait()
    for i in range(4):
        quarter(normed, i)
    z_hop(0, 2)
    z_hop(0, 1)
    z_hop(1, 1)
    z_hop(2, 1)
    quarter(tables, 0)
    quarter(tables, 1)
    y_hop(0, 2)
    y_hop(0, 1)
    z_hop(0, 4)
    z_hop(0, 3)
    x_hop(1, 1)
    z_hop(1, 2)
    z_hop(2, 2)
    quarter(tables, 2)
    quarter(tables, 3)
    y_hop(0, 4)
    y_hop(0, 3)
    z_hop(1, 3)
    z_hop(2, 3)
    p_hops(0)
    for c in range(chunks):
        keys_values(c)
        x_hop(1, 2) if c == 0 else y_hop(1, 1)
        for d in (0, 1):
            kv_copy(d, 0, c).start()
    x_hop(1, 3)
    z_hop(1, 4)
    z_hop(2, 4)
    y_hop(1, 2)
    x_hop(1, 4)
    y_hop(1, 3)
    x_hop(2, 1)
    x_hop(2, 2)
    y_hop(1, 4)
    x_hop(2, 3)
    x_hop(2, 4)
    p_hops(1)
    for c in range(chunks):
        here = pl.ds(c * CHUNK, CHUNK)
        for h in range(heads):
            q = _dot(a_s[here, :], wq_s[:, h * HEAD : (h + 1) * HEAD], 1, 0)
            q_s[pl.ds(h * own + c * CHUNK, CHUNK), :] = turned(q, here)

    for d in (0, 1):
        kv_arrival(d, 1, 0).wait_recv()
        kv_copy(d, 1, 0).start()

    block(z, 0, [p for p in pieces], [p for p in pieces if p % own < CHUNK], True)
    for c in range(1, chunks):
        block(z, c, [p for p in pieces if p % own >= c * CHUNK], [p for p in pieces if c * CHUNK <= p % own < (c + 1) * CHUNK], False)

    both = 2 * chunks * hops[1]

    def arrive(i, _):
        late = i >= both
        s = jnp.where(late, hops[0], 1 + lax.div(i, 2 * chunks))
        c = jnp.where(late, i - both, lax.div(lax.rem(i, 2 * chunks), 2))
        d = jnp.where(late, 0, lax.rem(i, 2))
        last = (d == 0) & (s == hops[0] - 1) & (c == chunks - 1)

        @pl.when(i >= 2)
        def _():
            kv_arrival(d, s, c).wait_recv()

        @pl.when((i >= 2) & (s < hops[0] - d) & jnp.logical_not(last))
        def _():
            kv_copy(d, s, c).start()

        @pl.when(last)
        def _():
            for part in range(2):
                kv_last(part, hops[0] - 1).start()

        @pl.when(i == 2)
        def _():
            for hop in range(1, hops[0] + 1):
                y_hop(2, hop)

        b = block_of(d, s)

        @pl.when(b < z)
        def _():
            block(b, c, [p for p in pieces], [], False)

    lax.fori_loop(0, both + chunks - 1, arrive, None)
    p_hops(2)
    b = block_of(0, hops[0])
    for part in range(2):
        kv_last(part, hops[0]).wait_recv()

        @pl.when(b < z)
        def _():
            block(b, chunks - 1, [p for p in pieces], [], False, (part,))

    for p in pieces:
        h, t = divmod(p, own)
        total = mix_s[HEAD : HEAD + 1, p : p + WIDE]
        seen_s[h * HEAD : (h + 1) * HEAD, t : t + WIDE] = (mix_s[:HEAD, p : p + WIDE] * (1 / total)).astype(jnp.bfloat16)

    for item in range(3):
        wait_all(item, 0 if item else 1, n - 1, z_send.at[item])
        if item:
            wait_all(item, 0, n - 1, x_send.at[item - 1])
        wait_all(item, 1, n - 1, y_send.at[item])
        wait_all(item, 2, n - 1, p_send.at[item])
    sent = kv_s.at[: n - 1]
    pltpu.make_async_copy(sent, sent, kv_send).wait()


def _project(x_ref, seen_ref, wo_ref, y_ref):
    here = pl.ds(pl.multiple_of(pl.program_id(0) * TILE, TILE), TILE)
    got = _dot(seen_ref[:, here], wo_ref[...], 0, 0)
    y_ref[...] = (x_ref[...].astype(jnp.float32) + got).astype(jnp.bfloat16)


def solution(mesh):
    n = mesh.shape["sp"]
    row = 2 * math.isqrt(mesh.shape["dp"] // 2)

    def step(x, gain, wq, wk, wv, wo):
        own, width = x.shape
        heads = wq.shape[1] // HEAD
        half = HEAD // 2
        freq = np.float32(THETA) ** (-np.arange(half, dtype=np.float32) / np.float32(half))
        bf, f32 = jnp.bfloat16, jnp.float32
        vmem = pl.BlockSpec(memory_space=pltpu.VMEM)
        hops = n // 2
        dma = pltpu.SemaphoreType.DMA
        seen, wo = pl.pallas_call(
            functools.partial(_kernel, n, row),
            name="attend",
            out_shape=[pltpu.VMEM((wq.shape[1], own), bf), pltpu.VMEM((wq.shape[1], width), bf)],
            in_specs=[pl.BlockSpec(memory_space=pltpu.HBM)] * 7,
            out_specs=[vmem, vmem],
            scratch_shapes=[
                pltpu.VMEM((own, width), bf),
                pltpu.VMEM((width,), bf),
                pltpu.VMEM((1, half), f32),
                pltpu.VMEM((own, width), bf),
                pltpu.VMEM((2, width, HEAD), bf),
                pltpu.VMEM((width, wq.shape[1]), bf),
                pltpu.VMEM((own, half), f32),
                pltpu.VMEM((own, half), f32),
                pltpu.VMEM((heads * own, HEAD), bf),
                pltpu.VMEM((n, own // CHUNK, CHUNK // PART, 2 * PART, HEAD), bf),
                pltpu.VMEM((1, heads * own), f32),
                pltpu.VMEM((HEAD + 8, heads * own), f32),
                dma((7,)),
                dma((3,)),
                dma((3, 2, hops)),
                dma((2,)),
                dma((2, hops)),
                dma((3,)),
                dma((3, hops)),
                dma((3,)),
                dma((3,)),
                dma,
                dma((2, hops, own // CHUNK)),
            ],
            compiler_params=pltpu.CompilerParams(collective_id=0, has_side_effects=True, vmem_limit_bytes=VMEM),
        )(*(pltpu.with_memory_space_constraint(t, pltpu.HBM) for t in (x, gain, jnp.asarray(freq[None]), wq, wk, wv, wo)))
        tile = pl.BlockSpec((TILE, width), lambda i: (i, 0))
        return pl.pallas_call(
            _project,
            name="project",
            out_shape=jax.ShapeDtypeStruct((own, width), bf),
            grid=(own // TILE,),
            in_specs=[tile, vmem, vmem],
            out_specs=tile,
            compiler_params=pltpu.CompilerParams(dimension_semantics=("arbitrary",), vmem_limit_bytes=16 * 2**20),
        )(x, seen, wo)

    tokens, whole = P(("dp", "sp"), None), P("sp", None)
    return jax.shard_map(
        step,
        mesh=mesh,
        in_specs=(tokens, P(None), whole, whole, whole, whole),
        out_specs=tokens,
        check_vma=False,
    )
```

```python
import functools
import math

import jax
import jax.numpy as jnp
import numpy as np
from jax import lax
from jax.experimental import pallas as pl
from jax.experimental.pallas import tpu as pltpu
from jax.sharding import PartitionSpec as P

HEAD = 256
THETA = 10000
MESH = pl.DeviceIdType.MESH
HIDDEN = -2e30
LOG2E = 1.4426950408889634
CHUNK = 512
PART = 256
WIDE = 512
TILE = 256
VMEM = 40 * 2**20


def _dot(a, b, ca, cb):
    return lax.dot_general(a, b, (((ca,), (cb,)), ((), ())), preferred_element_type=jnp.float32)


def _kernel(n, row, x_hbm, gain_hbm, freq_hbm, wq_hbm, wk_hbm, wv_hbm, wo_hbm, seen_s, wo_s,
            x_ref, gain_ref, freq_ref, a_s, wkv_s, wq_s, cos_s, sin_s, q_s, kv_s, top_s, mix_s,
            load_sem, z_send, z_recv, x_send, x_recv, y_send, y_recv, p_send, p_recv, kv_send, kv_recv):
    z = lax.axis_index("sp")
    dp = lax.axis_index("dp")
    core = lax.rem(dp, 2)
    ys = lax.rem(lax.div(dp, 2), 2)
    xs = lax.rem(lax.div(dp, row), 2)
    partner = dp + 1 - 2 * core
    across = dp + 2 - 4 * ys
    beside = dp + row - 2 * row * xs
    sign = 1 - 2 * core
    own = x_ref.shape[0]
    heads = wq_hbm.shape[1] // HEAD
    half = HEAD // 2
    cols = heads * own
    hops = (n // 2, n - 1 - n // 2)
    chunks = own // CHUNK

    def at(steps):
        return lax.rem(z + sign * steps + 2 * n, n)

    def step_of(d):
        return 1 - 2 * d

    rk, ro = wk_hbm.shape[0], wo_hbm.shape[0]
    own_rows = pl.ds(pl.multiple_of(z * rk, 16), rk)
    loads = [
        pltpu.make_async_copy(src, dst, load_sem.at[i])
        for i, (src, dst) in enumerate((
            (wk_hbm, wkv_s.at[0, own_rows, :]), (wv_hbm, wkv_s.at[1, own_rows, :]), (wq_hbm, wq_s.at[own_rows, :]),
            (wo_hbm, wo_s.at[pl.ds(pl.multiple_of(z * ro, 16), ro), :]), (gain_hbm, gain_ref), (freq_hbm, freq_ref), (x_hbm, x_ref)))
    ]
    for load in loads:
        load.start()

    barrier = pltpu.get_barrier_semaphore()
    greeted = [{"sp": at(k)} for k in (2, -2, 1, -1)] + [{"dp": partner}, {"dp": across}, {"dp": beside}]
    for target in greeted:
        pl.semaphore_signal(barrier, inc=1, device_id=target, device_id_type=MESH)
    pl.semaphore_wait(barrier, len(greeted))

    hq, ho = wq_hbm.shape[1] // 8, ro // 8

    def lot(c, y, x, level):
        return (4 * c + 2 * y + x, 1) if level == 0 else (4 * c + 2 * y, 2) if level == 1 else (4 * c, 4)

    def place(item, block, c, y, x, level):
        first, count = lot(c, y, x, level)
        if item == 0:
            here = pl.ds(pl.multiple_of(block * rk, 16), rk)
            return wkv_s.at[1 - c, here, :] if level == 2 else wkv_s.at[1 - c, here, pl.ds(pl.multiple_of(y * half, 128), half)]
        if item == 1:
            return wq_s.at[pl.ds(pl.multiple_of(block * rk, 16), rk), pl.ds(pl.multiple_of(first * hq, 128), count * hq)]
        return wo_s.at[pl.ds(pl.multiple_of(block * ro + first * ho, 16), count * ho), :]

    def copy(dst, send, recv, target):
        return pltpu.make_async_remote_copy(
            src_ref=dst, dst_ref=dst, send_sem=send, recv_sem=recv, device_id=target, device_id_type=MESH)

    def block_of(d, s):
        return at(-s * step_of(d))

    def group(s):
        return min(s, 3) - 1

    def z_copy(item, d, s):
        came = 0 if s <= 2 else 2
        return copy(place(item, block_of(d, came), core, ys, xs, 0), z_send.at[item], z_recv.at[item, group(s)],
                    {"sp": at(step_of(d) * (s - came))})

    def x_copy(item, d, s):
        return copy(place(item, block_of(d, s), core, ys, xs, 0), x_send.at[item - 1], x_recv.at[item - 1, int(s > 2)], {"dp": beside})

    def y_copy(item, d, s):
        return copy(place(item, block_of(d, s), core, ys, xs, 1), y_send.at[item], y_recv.at[item, int(s > 2)], {"dp": across})

    def p_copy(item, d, s):
        return copy(place(item, block_of(d, s), core, ys, xs, 2), p_send.at[item], p_recv.at[item], {"dp": partner})

    def some_of(item, level, count):
        if item == 0:
            return wkv_s.at[0, : count * rk, :] if level == 2 else wkv_s.at[0, : count * rk, :half]
        if item == 1:
            return wq_s.at[: count * rk, : hq << level]
        return wo_s.at[: count * (ho << level), :]

    def wait_all(item, level, count, sem):
        ref = some_of(item, level, count)
        pltpu.make_async_copy(ref, ref, sem).wait()

    near = [(d, s) for s in (2, 1) for d in (0, 1)]
    farther = [(d, s) for s in range(hops[0], 2, -1) for d in (0, 1) if s <= hops[d]]

    def own_w(item):
        for d, s in near:
            z_copy(item, d, s).start()

    def z_hop(item, g):
        these = [(d, s) for d, s in near + farther if group(s) == g]
        wait_all(item, 0, len(these), z_recv.at[item, g])
        if g == 1:
            for d, s in farther:
                z_copy(item, d, s).start()
        for d, s in these:
            (x_copy if item else y_copy)(item, d, s).start()

    def x_hop(item, late):
        these = farther if late else near
        wait_all(item, 0, len(these), x_recv.at[item - 1, late])
        for d, s in these:
            y_copy(item, d, s).start()

    def y_hop(item, late):
        these = farther if late else near
        wait_all(item, 1, len(these), y_recv.at[item, late])
        for d, s in these:
            p_copy(item, d, s).start()

    def p_hops(item):
        wait_all(item, 2, n - 1, p_recv.at[item])

    def wanted(d, s, here):
        up = lax.rem(core + d, 2) == 0
        return (up & (here >= s)) | (jnp.logical_not(up) & (lax.rem(here + s, n) < hops[0] - d))

    def sends(d, s):
        return wanted(d, s, at(step_of(d)))

    def kv_copy(d, s, c):
        return copy(kv_s.at[block_of(d, s), c], kv_send.at[d, s], kv_recv.at[d, s, c], {"sp": at(step_of(d))})

    def kv_arrival(d, s, c):
        return copy(kv_s.at[block_of(d, s), c], kv_send.at[d, s - 1], kv_recv.at[d, s - 1, c], {"sp": at(step_of(d))})

    def kv_own(values, c):
        ref = kv_s.at[z, c, :, PART:] if values else kv_s.at[z, c, :, :PART]
        for d in (0, 1):
            @pl.when(sends(d, 1))
            def _():
                copy(ref, kv_send.at[d, 0], kv_recv.at[d, 0, c], {"sp": at(step_of(d))}).start()

    def kv_last(i, s):
        return copy(kv_s.at[block_of(0, s), chunks - 1, i], kv_send.at[0, hops[0] - 1], kv_recv.at[1, hops[0] - 1, i],
                    {"sp": at(1)})

    rows = 128

    def normed(i, _):
        here = pl.ds(pl.multiple_of(i * rows, rows), rows)
        wide = x_ref[here, :].astype(jnp.float32)
        scale = lax.rsqrt(jnp.mean(wide * wide, -1, keepdims=True) + 1e-6)
        a_s[here, :] = (wide * scale * gain_ref[...].astype(jnp.float32).reshape(1, -1)).astype(jnp.bfloat16)

    def tables(i, _):
        here = pl.ds(pl.multiple_of(i * rows, rows), rows)
        token = lax.broadcasted_iota(jnp.int32, (rows, half), 0) + (z * own + i * rows)
        angle = token.astype(jnp.float32) * freq_ref[...]
        cos_s[here, :] = jnp.cos(angle)
        sin_s[here, :] = jnp.sin(angle)

    def turned(t, here):
        t = t.astype(jnp.bfloat16).astype(jnp.float32)
        a, b = t[:, :half], t[:, half:]
        cos, sin = cos_s[here, :], sin_s[here, :]
        return jnp.concatenate([a * cos - b * sin, b * cos + a * sin], axis=1).astype(jnp.bfloat16)

    def keys(c):
        here = pl.ds(c * CHUNK, CHUNK)
        k = turned(_dot(a_s[here, :], wkv_s[0], 1, 0), here)
        for i in range(CHUNK // PART):
            kv_s[z, c, i, :PART, :] = k[i * PART : (i + 1) * PART, :]

    def values(c):
        v = _dot(a_s[pl.ds(c * CHUNK, CHUNK), :], wkv_s[1], 1, 0).astype(jnp.bfloat16).T
        for i in range(CHUNK // PART):
            kv_s[z, c, i, PART:, :] = v[:, i * PART : (i + 1) * PART]

    e = HEAD**-0.5 * LOG2E
    pieces = range(0, cols, WIDE)

    def block(b, c, which, masked, first, parts=range(CHUNK // PART)):
        k = jnp.concatenate([kv_s[b, c, i, :PART, :] for i in parts], axis=0)
        v = jnp.concatenate([kv_s[b, c, i, PART:, :] for i in parts], axis=1)
        v = jnp.concatenate([v, jnp.ones((8, v.shape[1]), v.dtype)], axis=0)
        scores = [_dot(k, q_s[p : p + WIDE, :], 1, 1) for p in which]
        weights, keeps = [], []
        for p, s in zip(which, scores):
            if p in masked:
                key = lax.broadcasted_iota(jnp.int32, s.shape, 0) + c * CHUNK
                query = lax.broadcasted_iota(jnp.int32, s.shape, 1) + p % own
                s = jnp.where(query >= key, s, HIDDEN)
            top = s.max(axis=0, keepdims=True)
            if first:
                keeps.append(None)
            else:
                old = top_s[:, p : p + WIDE]
                top = jnp.maximum(old, top)
                keeps.append(jnp.exp2((old - top) * e))
            top_s[:, p : p + WIDE] = top
            weights.append(jnp.exp2((s - top) * e).astype(jnp.bfloat16))
        for p, w, keep in zip(which, weights, keeps):
            got = _dot(v, w, 1, 0)
            mix_s[:, p : p + WIDE] = got if first else mix_s[:, p : p + WIDE] * keep + got

    some = own // rows // 4

    def quarter(do, i):
        lax.fori_loop(i * some, (i + 1) * some, do, None)

    loads[0].wait()
    loads[1].wait()
    own_w(0)
    loads[2].wait()
    own_w(1)
    for load in loads[3:]:
        load.wait()
    for i in range(4):
        quarter(normed, i)
    quarter(tables, 0)
    quarter(tables, 1)
    z_hop(0, 1)
    z_hop(0, 0)
    own_w(2)
    quarter(tables, 2)
    z_hop(1, 1)
    z_hop(1, 0)
    quarter(tables, 3)
    y_hop(0, 0)
    z_hop(0, 2)
    z_hop(2, 1)
    z_hop(2, 0)

    @pl.when(core == 1)
    def _():
        y_hop(0, 1)

    @pl.when(core == 0)
    def _():
        p_hops(0)

    keys(0)
    x_hop(1, 0)
    kv_own(False, 0)

    @pl.when(core == 0)
    def _():
        y_hop(0, 1)

    z_hop(1, 2)
    for c in range(1, chunks):
        keys(c)
        kv_own(False, c)

    @pl.when(core == 1)
    def _():
        p_hops(0)

    for c in range(chunks):
        values(c)
        kv_own(True, c)
    x_hop(1, 1)
    y_hop(1, 0)
    z_hop(2, 2)
    y_hop(1, 1)
    x_hop(2, 0)
    x_hop(2, 1)
    p_hops(1)
    for c in range(chunks):
        here = pl.ds(c * CHUNK, CHUNK)
        for h in range(heads):
            q = _dot(a_s[here, :], wq_s[:, h * HEAD : (h + 1) * HEAD], 1, 0)
            q_s[pl.ds(h * own + c * CHUNK, CHUNK), :] = turned(q, here)

    block(z, 0, [p for p in pieces], [p for p in pieces if p % own < CHUNK], True)
    for d in (0, 1):
        @pl.when(wanted(d, 1, z))
        def _():
            kv_arrival(d, 1, 0).wait_recv()

        @pl.when(sends(d, 2))
        def _():
            kv_copy(d, 1, 0).start()

    for c in range(1, chunks):
        block(z, c, [p for p in pieces if p % own >= c * CHUNK], [p for p in pieces if c * CHUNK <= p % own < (c + 1) * CHUNK], False)

    both = 2 * chunks * hops[1]

    def arrive(i, _):
        late = i >= both
        s = jnp.where(late, hops[0], 1 + lax.div(i, 2 * chunks))
        c = jnp.where(late, i - both, lax.div(lax.rem(i, 2 * chunks), 2))
        d = jnp.where(late, 0, lax.rem(i, 2))
        last = (d == 0) & (s == hops[0] - 1) & (c == chunks - 1)

        @pl.when((i >= 2) & wanted(d, s, z))
        def _():
            kv_arrival(d, s, c).wait_recv()

        onward = (i >= 2) & (s < hops[0] - d) & sends(d, s + 1)

        @pl.when(onward & jnp.logical_not(last))
        def _():
            kv_copy(d, s, c).start()

        @pl.when(onward & last)
        def _():
            for part in range(2):
                kv_last(part, hops[0] - 1).start()

        @pl.when(i == 2)
        def _():
            y_hop(2, 0)
            y_hop(2, 1)

        b = block_of(d, s)

        @pl.when(b < z)
        def _():
            block(b, c, [p for p in pieces], [], False)

    lax.fori_loop(0, both + chunks - 1, arrive, None)
    p_hops(2)
    b = block_of(0, hops[0])
    for part in range(2):
        @pl.when(wanted(0, hops[0], z))
        def _():
            kv_last(part, hops[0]).wait_recv()

        @pl.when(b < z)
        def _():
            block(b, chunks - 1, [p for p in pieces], [], False, (part,))

    for p in pieces:
        h, t = divmod(p, own)
        total = mix_s[HEAD : HEAD + 1, p : p + WIDE]
        seen_s[h * HEAD : (h + 1) * HEAD, t : t + WIDE] = (mix_s[:HEAD, p : p + WIDE] * (1 / total)).astype(jnp.bfloat16)

    for item in range(3):
        wait_all(item, 0, n - 1, z_send.at[item])
        if item:
            wait_all(item, 0, n - 1, x_send.at[item - 1])
        wait_all(item, 1, n - 1, y_send.at[item])
        wait_all(item, 2, n - 1, p_send.at[item])
    for d in (0, 1):
        for s in range(hops[d]):
            @pl.when(sends(d, s + 1))
            def _():
                pltpu.make_async_copy(kv_s.at[0], kv_s.at[0], kv_send.at[d, s]).wait()


def _project(x_ref, seen_ref, wo_ref, y_hbm, y_ref, sem):
    own = x_ref.shape[0]
    done = []
    first = 0
    for i, size in enumerate((own // 2, own // 4, own // 8, own // 8)):
        for j in range(first, first + size, min(size, TILE)):
            here = slice(j, j + min(size, TILE))
            got = _dot(seen_ref[:, here], wo_ref[...], 0, 0)
            y_ref[here, :] = (x_ref[here, :].astype(jnp.float32) + got).astype(y_ref.dtype)
        here = slice(first, first + size)
        done.append(pltpu.make_async_copy(y_ref.at[here], y_hbm.at[here], sem.at[i]))
        done[-1].start()
        first += size
    for copy in done:
        copy.wait()


def solution(mesh):
    n = mesh.shape["sp"]
    row = 2 * math.isqrt(mesh.shape["dp"] // 2)

    def step(x, gain, wq, wk, wv, wo):
        own, width = x.shape
        heads = wq.shape[1] // HEAD
        half = HEAD // 2
        freq = np.float32(THETA) ** (-np.arange(half, dtype=np.float32) / np.float32(half))
        bf, f32 = jnp.bfloat16, jnp.float32
        vmem = pl.BlockSpec(memory_space=pltpu.VMEM)
        hops = n // 2
        dma = pltpu.SemaphoreType.DMA
        seen, wo = pl.pallas_call(
            functools.partial(_kernel, n, row),
            name="attend",
            out_shape=[pltpu.VMEM((wq.shape[1], own), bf), pltpu.VMEM((wq.shape[1], width), bf)],
            in_specs=[pl.BlockSpec(memory_space=pltpu.HBM)] * 7,
            out_specs=[vmem, vmem],
            scratch_shapes=[
                pltpu.VMEM((own, width), bf),
                pltpu.VMEM((width,), bf),
                pltpu.VMEM((1, half), f32),
                pltpu.VMEM((own, width), bf),
                pltpu.VMEM((2, width, HEAD), bf),
                pltpu.VMEM((width, wq.shape[1]), bf),
                pltpu.VMEM((own, half), f32),
                pltpu.VMEM((own, half), f32),
                pltpu.VMEM((heads * own, HEAD), bf),
                pltpu.VMEM((n, own // CHUNK, CHUNK // PART, 2 * PART, HEAD), bf),
                pltpu.VMEM((1, heads * own), f32),
                pltpu.VMEM((HEAD + 8, heads * own), f32),
                dma((7,)),
                dma((3,)),
                dma((3, 3)),
                dma((2,)),
                dma((2, 2)),
                dma((3,)),
                dma((3, 2)),
                dma((3,)),
                dma((3,)),
                dma((2, hops)),
                dma((2, hops, own // CHUNK)),
            ],
            compiler_params=pltpu.CompilerParams(collective_id=0, has_side_effects=True, vmem_limit_bytes=VMEM),
        )(*(pltpu.with_memory_space_constraint(t, pltpu.HBM) for t in (x, gain, jnp.asarray(freq[None]), wq, wk, wv, wo)))
        return pl.pallas_call(
            _project,
            name="project",
            out_shape=jax.ShapeDtypeStruct((own, width), bf),
            in_specs=[vmem] * 3,
            out_specs=pl.BlockSpec(memory_space=pltpu.HBM),
            scratch_shapes=[pltpu.VMEM((own, width), bf), dma((4,))],
            compiler_params=pltpu.CompilerParams(vmem_limit_bytes=16 * 2**20),
        )(x, seen, wo)

    tokens, whole = P(("dp", "sp"), None), P("sp", None)
    return jax.shard_map(
        step,
        mesh=mesh,
        in_specs=(tokens, P(None), whole, whole, whole, whole),
        out_specs=tokens,
        check_vma=False,
    )
```

```python
import functools
import math

import jax
import jax.numpy as jnp
import numpy as np
from jax import lax
from jax.experimental import pallas as pl
from jax.experimental.pallas import tpu as pltpu
from jax.sharding import PartitionSpec as P

HEAD = 256
THETA = 10000
MESH = pl.DeviceIdType.MESH
HIDDEN = -2e30
LOG2E = 1.4426950408889634
CHUNK = 512
PART = 256
WIDE = 512
TILE = 256
VMEM = 40 * 2**20


def _dot(a, b, ca, cb):
    return lax.dot_general(a, b, (((ca,), (cb,)), ((), ())), preferred_element_type=jnp.float32)


def _kernel(n, row, x_hbm, gain_hbm, freq_hbm, wq_hbm, wk_hbm, wv_hbm, wo_hbm, seen_s, wo_s,
            x_ref, gain_ref, freq_ref, a_s, wkv_s, wq_s, cos_s, sin_s, q_s, kv_s, top_s, mix_s,
            load_sem, z_send, z_recv, x_send, x_recv, y_send, y_recv, p_send, p_recv, kv_send, kv_recv):
    z = lax.axis_index("sp")
    dp = lax.axis_index("dp")
    core = lax.rem(dp, 2)
    ys = lax.rem(lax.div(dp, 2), 2)
    xs = lax.rem(lax.div(dp, row), 2)
    partner = dp + 1 - 2 * core
    across = dp + 2 - 4 * ys
    beside = dp + row - 2 * row * xs
    sign = 2 * core - 1
    own = x_ref.shape[0]
    heads = wq_hbm.shape[1] // HEAD
    half = HEAD // 2
    cols = heads * own
    hops = (n // 2, n - 1 - n // 2)
    chunks = own // CHUNK

    def at(steps):
        return lax.rem(z + sign * steps + 2 * n, n)

    def step_of(d):
        return 1 - 2 * d

    rk, ro = wk_hbm.shape[0], wo_hbm.shape[0]
    own_rows = pl.ds(pl.multiple_of(z * rk, 16), rk)
    loads = [
        pltpu.make_async_copy(src, dst, load_sem.at[i])
        for i, (src, dst) in enumerate((
            (wk_hbm, wkv_s.at[0, own_rows, :]), (wv_hbm, wkv_s.at[1, own_rows, :]), (wq_hbm, wq_s.at[own_rows, :]),
            (wo_hbm, wo_s.at[pl.ds(pl.multiple_of(z * ro, 16), ro), :]), (gain_hbm, gain_ref), (freq_hbm, freq_ref), (x_hbm, x_ref)))
    ]
    for load in loads:
        load.start()

    barrier = pltpu.get_barrier_semaphore()
    greeted = [{"sp": at(k)} for k in (2, -2, 1, -1)] + [{"dp": partner}, {"dp": across}, {"dp": beside}]
    for target in greeted:
        pl.semaphore_signal(barrier, inc=1, device_id=target, device_id_type=MESH)
    pl.semaphore_wait(barrier, len(greeted))

    hq, ho = wq_hbm.shape[1] // 8, ro // 8

    def lot(c, y, x, level):
        return (4 * c + 2 * y + x, 1) if level == 0 else (4 * c + 2 * y, 2) if level == 1 else (4 * c, 4)

    def place(item, block, c, y, x, level):
        first, count = lot(c, y, x, level)
        if item == 0:
            here = pl.ds(pl.multiple_of(block * rk, 16), rk)
            return wkv_s.at[1 - c, here, :] if level == 2 else wkv_s.at[1 - c, here, pl.ds(pl.multiple_of(y * half, 128), half)]
        if item == 1:
            return wq_s.at[pl.ds(pl.multiple_of(block * rk, 16), rk), pl.ds(pl.multiple_of(first * hq, 128), count * hq)]
        return wo_s.at[pl.ds(pl.multiple_of(block * ro + first * ho, 16), count * ho), :]

    def copy(dst, send, recv, target):
        return pltpu.make_async_remote_copy(
            src_ref=dst, dst_ref=dst, send_sem=send, recv_sem=recv, device_id=target, device_id_type=MESH)

    def block_of(d, s):
        return at(-s * step_of(d))

    def group(s):
        return min(s, 3) - 1

    def z_copy(item, d, s):
        came = 0 if s <= 2 else 2
        return copy(place(item, block_of(d, came), core, ys, xs, 0), z_send.at[item], z_recv.at[item, group(s)],
                    {"sp": at(step_of(d) * (s - came))})

    def x_copy(item, d, s):
        return copy(place(item, block_of(d, s), core, ys, xs, 0), x_send.at[item - 1], x_recv.at[item - 1, int(s > 2)], {"dp": beside})

    def y_copy(item, d, s):
        return copy(place(item, block_of(d, s), core, ys, xs, 1), y_send.at[item], y_recv.at[item, int(s > 2)], {"dp": across})

    def p_copy(item, d, s):
        return copy(place(item, block_of(d, s), core, ys, xs, 2), p_send.at[item], p_recv.at[item], {"dp": partner})

    def some_of(item, level, count):
        if item == 0:
            return wkv_s.at[0, : count * rk, :] if level == 2 else wkv_s.at[0, : count * rk, :half]
        if item == 1:
            return wq_s.at[: count * rk, : hq << level]
        return wo_s.at[: count * (ho << level), :]

    def wait_all(item, level, count, sem):
        ref = some_of(item, level, count)
        pltpu.make_async_copy(ref, ref, sem).wait()

    near = [(d, s) for s in (2, 1) for d in (0, 1)]
    farther = [(d, s) for s in range(hops[0], 2, -1) for d in (0, 1) if s <= hops[d]]

    def own_w(item):
        for d, s in near:
            z_copy(item, d, s).start()

    def z_hop(item, g):
        these = [(d, s) for d, s in near + farther if group(s) == g]
        wait_all(item, 0, len(these), z_recv.at[item, g])
        if g == 1:
            for d, s in farther:
                z_copy(item, d, s).start()
        for d, s in these:
            (x_copy if item else y_copy)(item, d, s).start()

    def x_hop(item, late):
        these = farther if late else near
        wait_all(item, 0, len(these), x_recv.at[item - 1, late])
        for d, s in these:
            y_copy(item, d, s).start()

    def y_hop(item, late):
        these = farther if late else near
        wait_all(item, 1, len(these), y_recv.at[item, late])
        for d, s in these:
            p_copy(item, d, s).start()

    def p_hops(item):
        wait_all(item, 2, n - 1, p_recv.at[item])

    def wanted(d, s, here):
        up = lax.rem(core + d, 2) == 1
        return (up & (here >= s)) | (jnp.logical_not(up) & (lax.rem(here + s, n) < hops[0] - d))

    def sends(d, s):
        return wanted(d, s, at(step_of(d)))

    def kv_copy(d, s, c):
        return copy(kv_s.at[block_of(d, s), c], kv_send.at[d, s], kv_recv.at[d, s, c], {"sp": at(step_of(d))})

    def kv_arrival(d, s, c):
        return copy(kv_s.at[block_of(d, s), c], kv_send.at[d, s - 1], kv_recv.at[d, s - 1, c], {"sp": at(step_of(d))})

    def kv_own(values, c):
        ref = kv_s.at[z, c, :, PART:] if values else kv_s.at[z, c, :, :PART]
        for d in (0, 1):
            @pl.when(sends(d, 1))
            def _():
                copy(ref, kv_send.at[d, 0], kv_recv.at[d, 0, c], {"sp": at(step_of(d))}).start()

    def kv_last(i, s):
        return copy(kv_s.at[block_of(0, s), chunks - 1, i], kv_send.at[0, hops[0] - 1], kv_recv.at[1, hops[0] - 1, i],
                    {"sp": at(1)})

    rows = 128

    def normed(i, _):
        here = pl.ds(pl.multiple_of(i * rows, rows), rows)
        wide = x_ref[here, :].astype(jnp.float32)
        scale = lax.rsqrt(jnp.mean(wide * wide, -1, keepdims=True) + 1e-6)
        a_s[here, :] = (wide * scale * gain_ref[...].astype(jnp.float32).reshape(1, -1)).astype(jnp.bfloat16)

    def tables(i, _):
        here = pl.ds(pl.multiple_of(i * rows, rows), rows)
        token = lax.broadcasted_iota(jnp.int32, (rows, half), 0) + (z * own + i * rows)
        angle = token.astype(jnp.float32) * freq_ref[...]
        cos_s[here, :] = jnp.cos(angle)
        sin_s[here, :] = jnp.sin(angle)

    def turned(t, here):
        t = t.astype(jnp.bfloat16).astype(jnp.float32)
        a, b = t[:, :half], t[:, half:]
        cos, sin = cos_s[here, :], sin_s[here, :]
        return jnp.concatenate([a * cos - b * sin, b * cos + a * sin], axis=1).astype(jnp.bfloat16)

    def keys(c):
        here = pl.ds(c * CHUNK, CHUNK)
        k = turned(_dot(a_s[here, :], wkv_s[0], 1, 0), here)
        for i in range(CHUNK // PART):
            kv_s[z, c, i, :PART, :] = k[i * PART : (i + 1) * PART, :]

    def values(c):
        v = _dot(a_s[pl.ds(c * CHUNK, CHUNK), :], wkv_s[1], 1, 0).astype(jnp.bfloat16).T
        for i in range(CHUNK // PART):
            kv_s[z, c, i, PART:, :] = v[:, i * PART : (i + 1) * PART]

    e = HEAD**-0.5 * LOG2E
    pieces = range(0, cols, WIDE)

    def block(b, c, which, masked, first, parts=range(CHUNK // PART)):
        k = jnp.concatenate([kv_s[b, c, i, :PART, :] for i in parts], axis=0)
        v = jnp.concatenate([kv_s[b, c, i, PART:, :] for i in parts], axis=1)
        v = jnp.concatenate([v, jnp.ones((8, v.shape[1]), v.dtype)], axis=0)
        scores = [_dot(k, q_s[p : p + WIDE, :], 1, 1) for p in which]
        weights, keeps = [], []
        for p, s in zip(which, scores):
            if p in masked:
                key = lax.broadcasted_iota(jnp.int32, s.shape, 0) + c * CHUNK
                query = lax.broadcasted_iota(jnp.int32, s.shape, 1) + p % own
                s = jnp.where(query >= key, s, HIDDEN)
            top = s.max(axis=0, keepdims=True)
            if first:
                keeps.append(None)
            else:
                old = top_s[:, p : p + WIDE]
                top = jnp.maximum(old, top)
                keeps.append(jnp.exp2((old - top) * e))
            top_s[:, p : p + WIDE] = top
            weights.append(jnp.exp2((s - top) * e).astype(jnp.bfloat16))
        for p, w, keep in zip(which, weights, keeps):
            got = _dot(v, w, 1, 0)
            mix_s[:, p : p + WIDE] = got if first else mix_s[:, p : p + WIDE] * keep + got

    some = own // rows // 4

    def quarter(do, i):
        lax.fori_loop(i * some, (i + 1) * some, do, None)

    loads[0].wait()
    loads[1].wait()
    own_w(0)
    loads[2].wait()
    own_w(1)
    for load in loads[3:]:
        load.wait()
    for i in range(4):
        quarter(normed, i)
    quarter(tables, 0)
    quarter(tables, 1)
    z_hop(0, 1)
    z_hop(0, 0)
    own_w(2)
    quarter(tables, 2)
    z_hop(1, 1)
    z_hop(1, 0)
    quarter(tables, 3)
    y_hop(0, 0)
    z_hop(0, 2)
    z_hop(2, 1)
    z_hop(2, 0)

    @pl.when(core == 1)
    def _():
        y_hop(0, 1)

    @pl.when(core == 0)
    def _():
        p_hops(0)

    keys(0)
    x_hop(1, 0)
    kv_own(False, 0)

    @pl.when(core == 0)
    def _():
        y_hop(0, 1)

    z_hop(1, 2)
    for c in range(1, chunks):
        keys(c)
        kv_own(False, c)

    @pl.when(core == 1)
    def _():
        p_hops(0)

    for c in range(chunks):
        values(c)
        kv_own(True, c)
    x_hop(1, 1)
    y_hop(1, 0)
    z_hop(2, 2)
    y_hop(1, 1)
    x_hop(2, 0)
    x_hop(2, 1)
    p_hops(1)
    for c in range(chunks):
        here = pl.ds(c * CHUNK, CHUNK)
        for h in range(heads):
            q = _dot(a_s[here, :], wq_s[:, h * HEAD : (h + 1) * HEAD], 1, 0)
            q_s[pl.ds(h * own + c * CHUNK, CHUNK), :] = turned(q, here)

    block(z, 0, [p for p in pieces], [p for p in pieces if p % own < CHUNK], True)
    for d in (0, 1):
        @pl.when(wanted(d, 1, z))
        def _():
            kv_arrival(d, 1, 0).wait_recv()

        @pl.when(sends(d, 2))
        def _():
            kv_copy(d, 1, 0).start()

    for c in range(1, chunks):
        block(z, c, [p for p in pieces if p % own >= c * CHUNK], [p for p in pieces if c * CHUNK <= p % own < (c + 1) * CHUNK], False)

    both = 2 * chunks * hops[1]

    def arrive(i, _):
        late = i >= both
        s = jnp.where(late, hops[0], 1 + lax.div(i, 2 * chunks))
        c = jnp.where(late, i - both, lax.div(lax.rem(i, 2 * chunks), 2))
        d = jnp.where(late, 0, lax.rem(i, 2))
        last = (d == 0) & (s == hops[0] - 1) & (c == chunks - 1)

        @pl.when((i >= 2) & wanted(d, s, z))
        def _():
            kv_arrival(d, s, c).wait_recv()

        onward = (i >= 2) & (s < hops[0] - d) & sends(d, s + 1)

        @pl.when(onward & jnp.logical_not(last))
        def _():
            kv_copy(d, s, c).start()

        @pl.when(onward & last)
        def _():
            for part in range(2):
                kv_last(part, hops[0] - 1).start()

        @pl.when(i == 2)
        def _():
            y_hop(2, 0)
            y_hop(2, 1)

        b = block_of(d, s)

        @pl.when(b < z)
        def _():
            block(b, c, [p for p in pieces], [], False)

    lax.fori_loop(0, both + chunks - 1, arrive, None)
    p_hops(2)
    b = block_of(0, hops[0])
    for part in range(2):
        @pl.when(wanted(0, hops[0], z))
        def _():
            kv_last(part, hops[0]).wait_recv()

        @pl.when(b < z)
        def _():
            block(b, chunks - 1, [p for p in pieces], [], False, (part,))

    for p in pieces:
        h, t = divmod(p, own)
        total = mix_s[HEAD : HEAD + 1, p : p + WIDE]
        seen_s[h * HEAD : (h + 1) * HEAD, t : t + WIDE] = (mix_s[:HEAD, p : p + WIDE] * (1 / total)).astype(jnp.bfloat16)

    for item in range(3):
        wait_all(item, 0, n - 1, z_send.at[item])
        if item:
            wait_all(item, 0, n - 1, x_send.at[item - 1])
        wait_all(item, 1, n - 1, y_send.at[item])
        wait_all(item, 2, n - 1, p_send.at[item])
    for d in (0, 1):
        for s in range(hops[d]):
            @pl.when(sends(d, s + 1))
            def _():
                pltpu.make_async_copy(kv_s.at[0], kv_s.at[0], kv_send.at[d, s]).wait()


def _project(x_ref, seen_ref, wo_ref, y_hbm, y_ref, sem):
    own = x_ref.shape[0]
    done = []
    first = 0
    for i, size in enumerate((own // 2, own // 4, own // 8, own // 8)):
        for j in range(first, first + size, min(size, TILE)):
            here = slice(j, j + min(size, TILE))
            got = _dot(seen_ref[:, here], wo_ref[...], 0, 0)
            y_ref[here, :] = (x_ref[here, :].astype(jnp.float32) + got).astype(y_ref.dtype)
        here = slice(first, first + size)
        done.append(pltpu.make_async_copy(y_ref.at[here], y_hbm.at[here], sem.at[i]))
        done[-1].start()
        first += size
    for copy in done:
        copy.wait()


def solution(mesh):
    n = mesh.shape["sp"]
    row = 2 * math.isqrt(mesh.shape["dp"] // 2)

    def step(x, gain, wq, wk, wv, wo):
        own, width = x.shape
        heads = wq.shape[1] // HEAD
        half = HEAD // 2
        freq = np.float32(THETA) ** (-np.arange(half, dtype=np.float32) / np.float32(half))
        bf, f32 = jnp.bfloat16, jnp.float32
        vmem = pl.BlockSpec(memory_space=pltpu.VMEM)
        hops = n // 2
        dma = pltpu.SemaphoreType.DMA
        seen, wo = pl.pallas_call(
            functools.partial(_kernel, n, row),
            name="attend",
            out_shape=[pltpu.VMEM((wq.shape[1], own), bf), pltpu.VMEM((wq.shape[1], width), bf)],
            in_specs=[pl.BlockSpec(memory_space=pltpu.HBM)] * 7,
            out_specs=[vmem, vmem],
            scratch_shapes=[
                pltpu.VMEM((own, width), bf),
                pltpu.VMEM((width,), bf),
                pltpu.VMEM((1, half), f32),
                pltpu.VMEM((own, width), bf),
                pltpu.VMEM((2, width, HEAD), bf),
                pltpu.VMEM((width, wq.shape[1]), bf),
                pltpu.VMEM((own, half), f32),
                pltpu.VMEM((own, half), f32),
                pltpu.VMEM((heads * own, HEAD), bf),
                pltpu.VMEM((n, own // CHUNK, CHUNK // PART, 2 * PART, HEAD), bf),
                pltpu.VMEM((1, heads * own), f32),
                pltpu.VMEM((HEAD + 8, heads * own), f32),
                dma((7,)),
                dma((3,)),
                dma((3, 3)),
                dma((2,)),
                dma((2, 2)),
                dma((3,)),
                dma((3, 2)),
                dma((3,)),
                dma((3,)),
                dma((2, hops)),
                dma((2, hops, own // CHUNK)),
            ],
            compiler_params=pltpu.CompilerParams(collective_id=0, has_side_effects=True, vmem_limit_bytes=VMEM),
        )(*(pltpu.with_memory_space_constraint(t, pltpu.HBM) for t in (x, gain, jnp.asarray(freq[None]), wq, wk, wv, wo)))
        return pl.pallas_call(
            _project,
            name="project",
            out_shape=jax.ShapeDtypeStruct((own, width), bf),
            in_specs=[vmem] * 3,
            out_specs=pl.BlockSpec(memory_space=pltpu.HBM),
            scratch_shapes=[pltpu.VMEM((own, width), bf), dma((4,))],
            compiler_params=pltpu.CompilerParams(vmem_limit_bytes=16 * 2**20),
        )(x, seen, wo)

    tokens, whole = P(("dp", "sp"), None), P("sp", None)
    return jax.shard_map(
        step,
        mesh=mesh,
        in_specs=(tokens, P(None), whole, whole, whole, whole),
        out_specs=tokens,
        check_vma=False,
    )
```
